32 devices in a mesh: section: 4 (over y, x), stem: 8 (over z, core).
Axes of the slice: x: 2, y: 2, z: 4, core: 2. Of those that a mesh axis runs over, the one named last changes fastest.
Arguments:
- bitstrings: int32 [4, 4, 32, 3], P('section'), may hold values 0 or 1
- boundary: float32 [2, 2048], replicated, may hold values from -6 to 6
- stem_tensor: float32 [4, 2, 2048, 8, 2048], P('section', None, 'stem'), may hold values from -0.09375 to 0.09375
- probe_vectors: float32 [4, 2, 2048], P('section'), may hold values from -0.09375 to 0.09375
- inbound_permutations: int32 [4, 2048], replicated, may hold values from 0 to 2047, each once within a row
Outputs:
- amplitudes: float32 [4, 2, 4, 32], P('section')
The draws below stay inside these ranges and needn't reach their ends.
Inputs may be any that keep to these rules, and one draw needn't show every extreme that they name: `inbound_permutations`: each row of relabeling names every number of 0 to 2047 once.
All inputs are finite; a program needn't handle non-finite values. No bound on the sum of `bitstrings` on one device may be relied on, other than what follows from the above.
Results may differ from the reference program's by a relative error of at most 0.0003.
Values sent between devices are 32-bit elements; how exact they have to be, the bound alone decides.
A program may use at most 128 MiB of HBM per device.

```python
import jax
import jax.numpy as jnp
from jax import lax

K = 2048
QS = 3
P_SIZE = 8
B = 32
M = 4
N_SECTION = 4


def touch_ends(array, rng, least, top_value):
    longest = array.shape.index(max(array.shape))
    spots = []
    for shift in (0, 1):
        where = [jax.random.randint(jax.random.fold_in(rng, axis), (), 0, length) for axis, length in enumerate(array.shape)]
        where[longest] = (where[longest] + shift) % array.shape[longest]
        spots.append(tuple(where))
    return array.at[spots[0]].set(least).at[spots[1]].set(top_value)


def levels(stream_key, dims, cuts, low, top_value):
    gain = 1.0
    for dim, shards_of in cuts:
        draws = jax.random.uniform(jax.random.fold_in(jax.random.fold_in(stream_key, 6), dim), (shards_of,), jnp.float32, low / len(cuts), top_value / len(cuts))
        gain = gain * jnp.repeat(jnp.exp(draws), dims[dim] // shards_of).reshape((-1,) + (1,) * (len(dims) - 1 - dim))
    return gain


def scatter_about(rng, dims, spread, limit, pieces=(), kind=jnp.bfloat16):
    values = spread * jax.random.normal(rng, dims, jnp.float32)
    if pieces:
        values = values * levels(rng, dims, pieces, -0.22, 0.18)
    return jnp.clip(values, -limit, limit).astype(kind)


def setup_inputs(seed: int = 0) -> dict:
    key_of = jax.random.split(jax.random.key(seed), 6)
    bitstrings = touch_ends((jax.random.randint(key_of[0], (N_SECTION, M, B, QS), 0, 2) < 1).astype(jnp.int32), jax.random.fold_in(key_of[0], 1), 0, 1)
    boundary = scatter_about(key_of[1], (2, K), 1.0, 6.0, (), jnp.float32)
    stem_tensor = scatter_about(key_of[2], (N_SECTION, 2, K, P_SIZE, K), (2 * K) ** -0.5, 0.09375, ((0, 4), (2, 8)), jnp.float32)
    probe_vectors = scatter_about(key_of[3], (N_SECTION, 2, K), (2 * K) ** -0.5, 0.09375, ((0, 4),), jnp.float32)
    inbound_permutations = jax.vmap(lambda own: jax.random.permutation(own, K))(jax.random.split(key_of[4], N_SECTION)).reshape((N_SECTION, K)).astype(jnp.int32)
    return {"bitstrings": bitstrings, "boundary": boundary, "stem_tensor": stem_tensor, "probe_vectors": probe_vectors, "inbound_permutations": inbound_permutations}


def reference(bitstrings, boundary, stem_tensor, probe_vectors, inbound_permutations):
    powers = (2 ** jnp.arange(QS)).astype(jnp.int32)
    configuration_line = jnp.sum(bitstrings * powers, axis=-1).astype(jnp.int32)
    running_partial_vector = jnp.broadcast_to(boundary[:, None, None, :], (2, M, B, K)).astype(jnp.float32)
    collected = []
    for segment_ordinal in range(N_SECTION):
        reordered_factor = jnp.take(running_partial_vector, inbound_permutations[segment_ordinal], axis=3)
        flat_real = stem_tensor[segment_ordinal, 0].reshape(K * P_SIZE, K)
        flat_imag = stem_tensor[segment_ordinal, 1].reshape(K * P_SIZE, K)

        def forward_group_move(pair):
            vectors, pattern = pair
            onehot = (jnp.arange(P_SIZE).astype(jnp.int32)[None, :] == pattern[:, None]).astype(jnp.float32)
            expanded = (vectors[:, :, :, None] * onehot[None, :, None, :]).reshape(2 * B, K * P_SIZE)
            prod_real = jnp.dot(expanded, flat_real, precision=lax.Precision.HIGHEST)
            prod_imag = jnp.dot(expanded, flat_imag, precision=lax.Precision.HIGHEST)
            out_real = prod_real[:B] - prod_imag[B:]
            out_imag = prod_imag[:B] + prod_real[B:]
            return jnp.stack([out_real, out_imag])

        permuted_entries = lax.map(forward_group_move, (jnp.transpose(reordered_factor, (1, 0, 2, 3)), configuration_line[segment_ordinal]))
        running_partial_vector = jnp.transpose(permuted_entries, (1, 0, 2, 3))
        probe_re = probe_vectors[segment_ordinal, 0]
        probe_im = probe_vectors[segment_ordinal, 1]
        amp_real = jnp.dot(running_partial_vector[0], probe_re, precision=lax.Precision.HIGHEST) - jnp.dot(running_partial_vector[1], probe_im, precision=lax.Precision.HIGHEST)
        amp_imag = jnp.dot(running_partial_vector[0], probe_im, precision=lax.Precision.HIGHEST) + jnp.dot(running_partial_vector[1], probe_re, precision=lax.Precision.HIGHEST)
        collected.append(jnp.stack([amp_real, amp_imag]))
    return jnp.stack(collected)
```

```python
import jax
import jax.numpy as jnp
from jax import lax
from jax.sharding import PartitionSpec as P

HIGH = lax.Precision.HIGH
HIGHEST = lax.Precision.HIGHEST


def halves(x):
    hi = lax.reduce_precision(x, 8, 7)
    return hi.astype(jnp.bfloat16), (x - hi).astype(jnp.bfloat16)


def select_columns(x, chosen):
    rows = x.shape[0]
    pick = (jnp.arange(x.shape[1], dtype=jnp.int32)[:, None] == chosen[None, :]).astype(jnp.bfloat16)
    hi, lo = halves(x)
    both = jnp.dot(jnp.concatenate([hi, lo]), pick, preferred_element_type=jnp.float32)
    return both[:rows] + both[rows:]


def local(bitstrings, boundary, stem_tensor, probe_vectors, inbound_permutations):
    section = lax.axis_index("section")
    sections = lax.axis_size("section")
    rank = lax.axis_index("stem")
    rows, settings, width = stem_tensor.shape[2:]
    bonds = boundary.shape[1]
    micro, batch, qubits = bitstrings.shape[1:]
    count = micro * batch
    powers = jnp.left_shift(jnp.int32(1), jnp.arange(qubits, dtype=jnp.int32))
    own_setting = jnp.sum(bitstrings[0] * powers, axis=-1).reshape(count)
    setting = lax.all_gather(own_setting, "section")
    probe = probe_vectors[0]
    perm = inbound_permutations

    def flat(plane):
        return stem_tensor[0, plane].reshape(rows * settings, width)

    def own_rows(row):
        return lax.dynamic_slice_in_dim(row, rank * rows, rows)

    zeros_a = jnp.zeros((2 * settings, bonds), jnp.float32)

    def first_forward():
        t_re, t_im = stem_tensor[0, 0], stem_tensor[0, 1]
        b = jnp.dot(
            boundary,
            (jnp.arange(bonds, dtype=jnp.int32)[:, None] == own_rows(perm[0])[None, :]).astype(jnp.float32),
            precision=HIGHEST,
        )
        b_re, b_im = b[0][:, None, None], b[1][:, None, None]
        u_re = jnp.sum(b_re * t_re - b_im * t_im, axis=0)
        u_im = jnp.sum(b_re * t_im + b_im * t_re, axis=0)
        return jnp.concatenate([u_re, u_im])

    def last_backward():
        t_re, t_im = stem_tensor[0, 0], stem_tensor[0, 1]
        v_re = jnp.sum(t_re * probe[0] - t_im * probe[1], axis=-1)
        v_im = jnp.sum(t_re * probe[1] + t_im * probe[0], axis=-1)
        v = jnp.concatenate([v_re.T, v_im.T])
        return lax.dynamic_update_slice_in_dim(zeros_a, v, rank * rows, 1)

    idle = lambda: zeros_a
    vectors = lax.switch(section, [first_forward, idle, idle, last_backward])

    def product_with_probe(v_re, v_im):
        return (
            jnp.dot(v_re, probe[0], precision=HIGHEST) - jnp.dot(v_im, probe[1], precision=HIGHEST),
            jnp.dot(v_re, probe[1], precision=HIGHEST) + jnp.dot(v_im, probe[0], precision=HIGHEST),
        )

    amp_first = jnp.stack(product_with_probe(vectors[:settings], vectors[settings:]))
    moved = lax.ppermute(vectors, "section", [(0, 1), (3, 2)])
    vectors = lax.psum(moved, "stem")

    ends = settings + 1
    pairs = settings * settings
    zeros_u = jnp.zeros((2 * pairs, bonds), jnp.float32)
    zeros_w = jnp.zeros((rows, settings * 2 * ends), jnp.float32)
    zeros_p = jnp.zeros((2, pairs), jnp.float32)

    def second_forward():
        x = select_columns(vectors, own_rows(perm[1])).reshape(2, settings, 1, rows, 1)
        same = jnp.eye(settings, dtype=jnp.float32).reshape(1, 1, settings, 1, settings)
        spread = (x * same).reshape(2 * pairs, rows * settings)
        p_re = jnp.dot(spread, flat(0), precision=HIGH)
        p_im = jnp.dot(spread, flat(1), precision=HIGH)
        u_re = p_re[:pairs] - p_im[pairs:]
        u_im = p_im[:pairs] + p_re[pairs:]
        amp = jnp.stack(product_with_probe(u_re, u_im))
        u = select_columns(jnp.concatenate([u_re, u_im]), perm[2])
        return u, zeros_w, amp

    def second_backward():
        place = (perm[3][:, None] == jnp.arange(bonds, dtype=jnp.int32)[None, :]).astype(jnp.bfloat16)
        hi, lo = halves(vectors)
        both = jnp.dot(jnp.concatenate([hi, lo]), place, preferred_element_type=jnp.float32)
        v = (both[: 2 * settings] + both[2 * settings :]).reshape(2, settings, bonds)
        v = jnp.concatenate([v, probe[:, None, :]], axis=1).reshape(2 * ends, bonds)
        q_re = lax.dot_general(flat(0), v, (((1,), (1,)), ((), ())), precision=HIGH)
        q_im = lax.dot_general(flat(1), v, (((1,), (1,)), ((), ())), precision=HIGH)
        w_re = q_re[:, :ends] - q_im[:, ends:]
        w_im = q_re[:, ends:] + q_im[:, :ends]
        w = jnp.concatenate([w_re, w_im], axis=1).reshape(rows, settings * 2 * ends)
        return zeros_u, w, zeros_p

    none = lambda: (zeros_u, zeros_w, zeros_p)
    u, w, amp_second = lax.switch(section, [none, second_forward, second_backward, none])
    w = lax.ppermute(w, "section", [(2, 1)])
    w = lax.all_gather(w, "stem", axis=0, tiled=True)
    joined = jnp.dot(u, w, precision=HIGH).reshape(2, pairs, settings, 2, ends)
    j_re = (joined[0, :, :, 0] - joined[1, :, :, 1]).reshape(pairs, settings * ends)
    j_im = (joined[0, :, :, 1] + joined[1, :, :, 0]).reshape(pairs, settings * ends)

    onehot = lambda ids, size: (ids[:, None] == jnp.arange(size, dtype=jnp.int32)[None, :]).astype(jnp.float32)
    front = onehot(setting[0] * settings + setting[1], pairs)
    first = jnp.dot(amp_first, onehot(setting[0], settings).T, precision=HIGHEST)
    first = jnp.where(section == 0, first, 0.0)
    second = jnp.dot(amp_second, front.T, precision=HIGHEST)
    third_pick = onehot(setting[2] * ends + settings, settings * ends)
    fourth_pick = onehot(setting[2] * ends + setting[3], settings * ends)
    rows_re = jnp.dot(front, j_re, precision=HIGHEST)
    rows_im = jnp.dot(front, j_im, precision=HIGHEST)
    third = jnp.stack([jnp.sum(rows_re * third_pick, axis=1), jnp.sum(rows_im * third_pick, axis=1)])
    fourth = jnp.stack([jnp.sum(rows_re * fourth_pick, axis=1), jnp.sum(rows_im * fourth_pick, axis=1)])
    partial = jnp.stack([first, second, third, fourth])
    total = lax.psum(partial, ("section", "stem"))
    own = lax.dynamic_index_in_dim(total, section, 0, False)
    return own.reshape(1, 2, micro, batch)


def solution(mesh):
    return jax.shard_map(
        local,
        mesh=mesh,
        in_specs=(
            P("section", None, None, None),
            P(),
            P("section", None, "stem", None, None),
            P("section", None, None),
            P(),
        ),
        out_specs=P("section", None, None, None),
        check_vma=False,
    )
```

```python
import functools

import jax
import jax.numpy as jnp
from jax import lax
from jax.experimental import pallas as pl
from jax.experimental.pallas import tpu as pltpu
from jax.sharding import PartitionSpec as P

HIGH = lax.Precision.HIGH
HIGHEST = lax.Precision.HIGHEST


def halves(x):
    hi = lax.reduce_precision(x, 8, 7)
    return hi.astype(jnp.bfloat16), (x - hi).astype(jnp.bfloat16)


def select_columns(x, chosen):
    rows = x.shape[0]
    pick = (jnp.arange(x.shape[1], dtype=jnp.int32)[:, None] == chosen[None, :]).astype(jnp.bfloat16)
    hi, lo = halves(x)
    both = jnp.dot(jnp.concatenate([hi, lo]), pick, preferred_element_type=jnp.float32)
    return both[:rows] + both[rows:]


MESH = pl.DeviceIdType.MESH
VMEM = pl.BlockSpec(memory_space=pltpu.VMEM)


def send(src, dst, send_sem, recv_sem, target):
    return pltpu.make_async_remote_copy(
        src_ref=src, dst_ref=dst, send_sem=send_sem, recv_sem=recv_sem, device_id=target, device_id_type=MESH
    )


def greet(targets):
    barrier = pltpu.get_barrier_semaphore()
    for target in targets:
        pl.semaphore_signal(barrier, inc=1, device_id=target, device_id_type=MESH)
    pl.semaphore_wait(barrier, len(targets))


def call(kernel, outs, scratch, collective_id, *args):
    return pl.pallas_call(
        kernel,
        out_shape=[jax.ShapeDtypeStruct(shape, jnp.float32) for shape in outs],
        in_specs=[VMEM] * len(args),
        out_specs=[VMEM] * len(outs),
        scratch_shapes=scratch,
        compiler_params=pltpu.CompilerParams(collective_id=collective_id, has_side_effects=True),
    )(*args)


def exchange_kernel(S, R, v_ref, set_ref, out_ref, sets_ref, land, total, s1, r1, s2, r2, s3, r3):
    me_s, me_r = lax.axis_index("section"), lax.axis_index("stem")
    partner = me_s + 1 - 2 * (me_s % 2)
    ranks = [(me_r + d) % R for d in range(R)]
    others = [(me_s + d) % S for d in range(S)]
    greet(
        [(me_s, r) for r in ranks[1:]] + [(partner, r) for r in ranks] + [(s, me_r) for s in others[1:]]
    )
    first = [
        send(v_ref.at[ranks[d]], land.at[d - 1], s1.at[d - 1], r1.at[d - 1], (me_s, ranks[d])) for d in range(1, R)
    ]
    third = [
        send(set_ref, sets_ref.at[me_s], s3.at[d - 1], r3.at[d - 1], (others[d], me_r)) for d in range(1, S)
    ]
    for copy in first + third:
        copy.start()
    sets_ref[me_s] = set_ref[...]
    value = v_ref[me_r]
    for d in range(1, R):
        first[d - 1].wait_recv()
        value = value + land[d - 1]
    total[...] = value
    second = [send(total, out_ref.at[me_r], s2.at[d], r2.at[d], (partner, ranks[d])) for d in range(R)]
    for copy in second:
        copy.start()
    for copy in first:
        copy.wait_send()
    for copy in second + third:
        copy.wait()


def exchange(S, R, v, sets):
    return call(
        functools.partial(exchange_kernel, S, R),
        [v.shape, (S,) + sets.shape],
        [
            pltpu.VMEM((R - 1,) + v.shape[1:], jnp.float32),
            pltpu.VMEM(v.shape[1:], jnp.float32),
            pltpu.SemaphoreType.DMA((R - 1,)),
            pltpu.SemaphoreType.DMA((R - 1,)),
            pltpu.SemaphoreType.DMA((R,)),
            pltpu.SemaphoreType.DMA((R,)),
            pltpu.SemaphoreType.DMA((S - 1,)),
            pltpu.SemaphoreType.DMA((S - 1,)),
        ],
        1,
        v,
        sets,
    )


def meet_kernel(S, R, u_ref, w_ref, sum_ref, out_ref, land, su, ru, sw, rw):
    me_s, me_r = lax.axis_index("section"), lax.axis_index("stem")
    ranks = [(me_r + d) % R for d in range(R)]
    greet([((me_s + e) % S, ranks[d]) for e in range(S) for d in range(R) if e + d])
    far = [s for s in range(S) if s != 1]

    def u_copies():
        return [
            send(u_ref.at[ranks[d] * S + s], land.at[me_r], su.at[d * S + s], ru.at[me_r], (s, ranks[d]))
            for d in range(R)
            for s in range(S)
            if s != 1 or d
        ]

    def w_copies():
        return [send(w_ref.at[s], out_ref, sw.at[s], rw.at[0], (s, me_r)) for s in range(S) if s != 2]

    def arrived(rank):
        send(land.at[rank], land.at[rank], su.at[0], ru.at[rank], (me_s, ranks[1])).wait_recv()

    @pl.when(me_s == 1)
    def _():
        for copy in u_copies():
            copy.start()
        land[me_r] = u_ref[me_r * S + 1]

    @pl.when(me_s == 2)
    def _():
        for copy in w_copies():
            copy.start()
        out_ref[...] = w_ref[2]

    @pl.when(me_s == 1)
    def _():
        for d in range(1, R):
            arrived(ranks[d])
        for copy in u_copies():
            copy.wait_send()

    @pl.when(me_s != 1)
    def _():
        for rank in range(R):
            arrived(rank)

    @pl.when(me_s == 2)
    def _():
        for copy in w_copies():
            copy.wait_send()

    @pl.when(me_s != 2)
    def _():
        send(out_ref, out_ref, sw.at[0], rw.at[0], (me_s, ranks[1])).wait_recv()

    value = land[0]
    for rank in range(1, R):
        value = value + land[rank]
    sum_ref[...] = value


def meet(S, R, u, w):
    return call(
        functools.partial(meet_kernel, S, R),
        [u.shape[1:], w.shape[1:]],
        [
            pltpu.VMEM((R,) + u.shape[1:], jnp.float32),
            pltpu.SemaphoreType.DMA((S * R,)),
            pltpu.SemaphoreType.DMA((R,)),
            pltpu.SemaphoreType.DMA((S,)),
            pltpu.SemaphoreType.DMA((1,)),
        ],
        2,
        u,
        w,
    )


def total_kernel(S, R, p_ref, out_ref, land, half, far, s1, r1, s2, r2):
    me_s, me_r = lax.axis_index("section"), lax.axis_index("stem")
    near = [(me_s, (me_r + d) % R) for d in range(1, R)]
    across = [((me_s + d) % S, me_r) for d in range(1, S)]
    greet(near + across)
    first = [send(p_ref, land.at[d], s1.at[d], r1.at[d], near[d]) for d in range(R - 1)]
    for copy in first:
        copy.start()
    value = p_ref[...]
    for d in range(R - 1):
        first[d].wait_recv()
        value = value + land[d]
    half[...] = value
    second = [send(half, far.at[d], s2.at[d], r2.at[d], across[d]) for d in range(S - 1)]
    for copy in second:
        copy.start()
    for d in range(S - 1):
        second[d].wait_recv()
        value = value + far[d]
    out_ref[...] = value
    for copy in first + second:
        copy.wait_send()


def total(S, R, p):
    return call(
        functools.partial(total_kernel, S, R),
        [p.shape],
        [
            pltpu.VMEM((R - 1,) + p.shape, jnp.float32),
            pltpu.VMEM(p.shape, jnp.float32),
            pltpu.VMEM((S - 1,) + p.shape, jnp.float32),
            pltpu.SemaphoreType.DMA((R - 1,)),
            pltpu.SemaphoreType.DMA((R - 1,)),
            pltpu.SemaphoreType.DMA((S - 1,)),
            pltpu.SemaphoreType.DMA((S - 1,)),
        ],
        3,
        p,
    )[0]


def local(bitstrings, boundary, stem_tensor, probe_vectors, inbound_permutations):
    section = lax.axis_index("section")
    sections = lax.axis_size("section")
    rank = lax.axis_index("stem")
    rows, settings, width = stem_tensor.shape[2:]
    bonds = boundary.shape[1]
    micro, batch, qubits = bitstrings.shape[1:]
    count = micro * batch
    powers = jnp.left_shift(jnp.int32(1), jnp.arange(qubits, dtype=jnp.int32))
    own_setting = jnp.sum(bitstrings[0] * powers, axis=-1).reshape(count)
    ranks = lax.axis_size("stem")
    probe = probe_vectors[0]
    perm = inbound_permutations

    def flat(plane):
        return stem_tensor[0, plane].reshape(rows * settings, width)

    def own_rows(row):
        return lax.dynamic_slice_in_dim(row, rank * rows, rows)

    zeros_a = jnp.zeros((2 * settings, bonds), jnp.float32)

    def first_forward():
        t_re, t_im = stem_tensor[0, 0], stem_tensor[0, 1]
        b = jnp.dot(
            boundary,
            (jnp.arange(bonds, dtype=jnp.int32)[:, None] == own_rows(perm[0])[None, :]).astype(jnp.float32),
            precision=HIGHEST,
        )
        b_re, b_im = b[0][:, None, None], b[1][:, None, None]
        u_re = jnp.sum(b_re * t_re - b_im * t_im, axis=0)
        u_im = jnp.sum(b_re * t_im + b_im * t_re, axis=0)
        return jnp.concatenate([u_re, u_im])

    def last_backward():
        t_re, t_im = stem_tensor[0, 0], stem_tensor[0, 1]
        v_re = jnp.sum(t_re * probe[0] - t_im * probe[1], axis=-1)
        v_im = jnp.sum(t_re * probe[1] + t_im * probe[0], axis=-1)
        v = jnp.concatenate([v_re.T, v_im.T])
        return lax.dynamic_update_slice_in_dim(zeros_a, v, rank * rows, 1)

    idle = lambda: zeros_a
    vectors = lax.switch(section, [first_forward, idle, idle, last_backward])

    def product_with_probe(v_re, v_im):
        return (
            jnp.dot(v_re, probe[0], precision=HIGHEST) - jnp.dot(v_im, probe[1], precision=HIGHEST),
            jnp.dot(v_re, probe[1], precision=HIGHEST) + jnp.dot(v_im, probe[0], precision=HIGHEST),
        )

    amp_first = jnp.stack(product_with_probe(vectors[:settings], vectors[settings:]))
    blocks = vectors.reshape(2 * settings, ranks, rows).transpose(1, 0, 2)
    own_block = jnp.broadcast_to(own_setting.astype(jnp.float32), (8, count))
    blocks, setting = exchange(sections, ranks, blocks, own_block)
    setting = setting[:, 0].astype(jnp.int32)
    vectors = blocks.transpose(1, 0, 2).reshape(2 * settings, bonds)

    ends = settings + 1
    pairs = settings * settings
    zeros_u = jnp.zeros((bonds, 2 * pairs), jnp.float32)
    zeros_w = jnp.zeros((rows, 4 * pairs), jnp.float32)
    zeros_p = jnp.zeros((2, pairs), jnp.float32)

    def second_forward():
        x = select_columns(vectors, jnp.repeat(own_rows(perm[1]), settings))
        same = jnp.arange(rows * settings, dtype=jnp.int32)[None, :] % settings
        same = (same == jnp.arange(settings, dtype=jnp.int32)[:, None]).astype(jnp.float32)
        spread = (x[:, None, :] * same[None]).reshape(2 * pairs, rows * settings)
        p_re = jnp.dot(spread, flat(0), precision=HIGH)
        p_im = jnp.dot(spread, flat(1), precision=HIGH)
        u_re = p_re[:pairs] - p_im[pairs:]
        u_im = p_im[:pairs] + p_re[pairs:]
        amp = jnp.stack(product_with_probe(u_re, u_im))
        hi, lo = halves(jnp.concatenate([u_re, u_im]))
        pick = (perm[2][:, None] == jnp.arange(bonds, dtype=jnp.int32)[None, :]).astype(jnp.bfloat16)
        both = lax.dot_general(
            pick, jnp.concatenate([hi, lo]), (((1,), (1,)), ((), ())), preferred_element_type=jnp.float32
        )
        return both[:, : 2 * pairs] + both[:, 2 * pairs :], zeros_w, amp

    def second_backward():
        place = (perm[3][:, None] == jnp.arange(bonds, dtype=jnp.int32)[None, :]).astype(jnp.bfloat16)
        hi, lo = halves(vectors)
        both = jnp.dot(jnp.concatenate([hi, lo]), place, preferred_element_type=jnp.float32)
        v = (both[: 2 * settings] + both[2 * settings :]).reshape(2, settings, bonds)
        v = jnp.concatenate([v, probe[:, None, :]], axis=1).reshape(2 * ends, bonds)
        q_re = lax.dot_general(flat(0), v, (((1,), (1,)), ((), ())), precision=HIGH)
        q_im = lax.dot_general(flat(1), v, (((1,), (1,)), ((), ())), precision=HIGH)
        w_re = q_re[:, :ends] - q_im[:, ends:]
        w_im = q_re[:, ends:] + q_im[:, :ends]
        w_re, w_im = w_re.reshape(rows, settings, ends), w_im.reshape(rows, settings, ends)
        w = jnp.concatenate(
            [
                w_re[:, :, :settings].reshape(rows, pairs),
                w_im[:, :, :settings].reshape(rows, pairs),
                w_re[:, :, settings],
                w_im[:, :, settings],
                jnp.zeros((rows, 2 * pairs - 2 * settings), jnp.float32),
            ],
            axis=1,
        )
        return zeros_u, w, zeros_p

    none = lambda: (zeros_u, zeros_w, zeros_p)
    u, w, amp_second = lax.switch(section, [none, second_forward, second_backward, none])
    share = rows // sections
    u, w = meet(
        sections, ranks, u.reshape(sections * ranks, share, 2 * pairs), w.reshape(sections, share, 4 * pairs)
    )
    joined = lax.dot_general(u, w, (((0,), (0,)), ((), ())), precision=HIGHEST)
    upper, lower = joined[:pairs], joined[pairs:]
    far_re = upper[:, :pairs] - lower[:, pairs : 2 * pairs]
    far_im = upper[:, pairs : 2 * pairs] + lower[:, :pairs]
    near = joined[:, 2 * pairs :]
    near_re = near[:pairs, :settings] - near[pairs:, settings : 2 * settings]
    near_im = near[:pairs, settings : 2 * settings] + near[pairs:, :settings]

    onehot = lambda ids, size: (ids[:, None] == jnp.arange(size, dtype=jnp.int32)[None, :]).astype(jnp.float32)
    front = onehot(setting[0] * settings + setting[1], pairs)
    first = jnp.dot(amp_first, onehot(setting[0], settings).T, precision=HIGHEST)
    first = jnp.where(section == 0, first, 0.0)
    second = jnp.dot(amp_second, front.T, precision=HIGHEST)
    third_pick = onehot(setting[2], settings)
    fourth_pick = onehot(setting[2] * settings + setting[3], pairs)

    def chosen(table, pick):
        return jnp.sum(jnp.dot(front, table, precision=HIGHEST) * pick, axis=1)

    third = jnp.stack([chosen(near_re, third_pick), chosen(near_im, third_pick)])
    fourth = jnp.stack([chosen(far_re, fourth_pick), chosen(far_im, fourth_pick)])
    partial = jnp.stack([first, second, third, fourth]).reshape(2 * sections, count)
    summed = total(sections, ranks, partial).reshape(sections, 2, count)
    own = lax.dynamic_index_in_dim(summed, section, 0, False)
    return own.reshape(1, 2, micro, batch)


def solution(mesh):
    return jax.shard_map(
        local,
        mesh=mesh,
        in_specs=(
            P("section", None, None, None),
            P(),
            P("section", None, "stem", None, None),
            P("section", None, None),
            P(),
        ),
        out_specs=P("section", None, None, None),
        check_vma=False,
    )
```

```python
import functools

import jax
import jax.numpy as jnp
from jax import lax
from jax.experimental import pallas as pl
from jax.experimental.pallas import tpu as pltpu
from jax.sharding import PartitionSpec as P

HIGH = lax.Precision.HIGH
HIGHEST = lax.Precision.HIGHEST


def halves(x):
    hi = lax.reduce_precision(x, 8, 7)
    return hi.astype(jnp.bfloat16), (x - hi).astype(jnp.bfloat16)


def select_columns(x, chosen):
    rows = x.shape[0]
    pick = (jnp.arange(x.shape[1], dtype=jnp.int32)[:, None] == chosen[None, :]).astype(jnp.bfloat16)
    hi, lo = halves(x)
    both = jnp.dot(jnp.concatenate([hi, lo]), pick, preferred_element_type=jnp.float32)
    return both[:rows] + both[rows:]


MESH = pl.DeviceIdType.MESH
VMEM = pl.BlockSpec(memory_space=pltpu.VMEM)


def send(src, dst, send_sem, recv_sem, target):
    return pltpu.make_async_remote_copy(
        src_ref=src, dst_ref=dst, send_sem=send_sem, recv_sem=recv_sem, device_id=target, device_id_type=MESH
    )


def greet(targets):
    barrier = pltpu.get_barrier_semaphore()
    for target in targets:
        pl.semaphore_signal(barrier, inc=1, device_id=target, device_id_type=MESH)
    pl.semaphore_wait(barrier, len(targets))


def call(kernel, outs, scratch, collective_id, *args):
    return pl.pallas_call(
        kernel,
        out_shape=[jax.ShapeDtypeStruct(shape, jnp.float32) for shape in outs],
        in_specs=[VMEM] * len(args),
        out_specs=[VMEM] * len(outs),
        scratch_shapes=scratch,
        compiler_params=pltpu.CompilerParams(collective_id=collective_id, has_side_effects=True),
    )(*args)


def exchange_kernel(S, R, v_ref, set_ref, out_ref, sets_ref, land, total, s1, r1, s2, r2, s3, r3):
    me_s, me_r = lax.axis_index("section"), lax.axis_index("stem")
    partner = me_s + 1 - 2 * (me_s % 2)
    ranks = [(me_r + d) % R for d in range(R)]
    others = [(me_s + d) % S for d in range(S)]
    greet(
        [(me_s, r) for r in ranks[1:]] + [(partner, r) for r in ranks] + [(s, me_r) for s in others[1:]]
    )
    first = [
        send(v_ref.at[ranks[d]], land.at[d - 1], s1.at[d - 1], r1.at[d - 1], (me_s, ranks[d])) for d in range(1, R)
    ]
    third = [
        send(set_ref, sets_ref.at[me_s], s3.at[d - 1], r3.at[d - 1], (others[d], me_r)) for d in range(1, S)
    ]
    for copy in first + third:
        copy.start()
    sets_ref[me_s] = set_ref[...]
    value = v_ref[me_r]
    for d in range(1, R):
        first[d - 1].wait_recv()
        value = value + land[d - 1]
    total[...] = value
    second = [send(total, out_ref.at[me_r], s2.at[d], r2.at[d], (partner, ranks[d])) for d in range(R)]
    for copy in second:
        copy.start()
    for copy in first:
        copy.wait_send()
    for copy in second + third:
        copy.wait()


def exchange(S, R, v, sets):
    return call(
        functools.partial(exchange_kernel, S, R),
        [v.shape, (S,) + sets.shape],
        [
            pltpu.VMEM((R - 1,) + v.shape[1:], jnp.float32),
            pltpu.VMEM(v.shape[1:], jnp.float32),
            pltpu.SemaphoreType.DMA((R - 1,)),
            pltpu.SemaphoreType.DMA((R - 1,)),
            pltpu.SemaphoreType.DMA((R,)),
            pltpu.SemaphoreType.DMA((R,)),
            pltpu.SemaphoreType.DMA((S - 1,)),
            pltpu.SemaphoreType.DMA((S - 1,)),
        ],
        1,
        v,
        sets,
    )


def meet_kernel(
    S, R, u_ref, w_ref, f_ref, g_ref, h_ref, e_ref, sum_ref, land, out_ref, su, ru, sw, rw,
    part, land1, half, far, s1, r1, s2, r2,
):
    me_s, me_r = lax.axis_index("section"), lax.axis_index("stem")
    ranks = [(me_r + d) % R for d in range(R)]
    greet([((me_s + e) % S, ranks[d]) for e in range(S) for d in range(R) if e + d])
    def u_copies():
        return [
            send(u_ref.at[ranks[d] * S + s], land.at[me_r], su.at[d * S + s], ru.at[me_r], (s, ranks[d]))
            for d in range(R)
            for s in range(S)
            if s != 1 or d
        ]

    def w_copies():
        return [send(w_ref.at[s], out_ref, sw.at[s], rw.at[0], (s, me_r)) for s in range(S) if s != 2]

    def arrived(rank):
        send(land.at[rank], land.at[rank], su.at[0], ru.at[rank], (me_s, ranks[1])).wait_recv()

    @pl.when(me_s == 1)
    def _():
        for copy in u_copies():
            copy.start()
        land[me_r] = u_ref[me_r * S + 1]

    @pl.when(me_s == 2)
    def _():
        for copy in w_copies():
            copy.start()
        out_ref[...] = w_ref[2]

    @pl.when(me_s == 1)
    def _():
        for d in range(1, R):
            arrived(ranks[d])
        for copy in u_copies():
            copy.wait_send()

    @pl.when(me_s != 1)
    def _():
        for rank in range(R):
            arrived(rank)

    @pl.when(me_s == 2)
    def _():
        for copy in w_copies():
            copy.wait_send()

    @pl.when(me_s != 2)
    def _():
        send(out_ref, out_ref, sw.at[0], rw.at[0], (me_s, ranks[1])).wait_recv()

    value = land[0]
    for rank in range(1, R):
        value = value + land[rank]

    def dot(a, b):
        return jnp.dot(a, b, precision=HIGHEST, preferred_element_type=jnp.float32)

    def put(row, a, b):
        n = a.shape[1] // 2
        part[row : row + 1, :] = jnp.sum(a[:, :n] * b[:, :n] - a[:, n:] * b[:, n:], axis=0, keepdims=True)
        part[row + 1 : row + 2, :] = jnp.sum(a[:, :n] * b[:, n:] + a[:, n:] * b[:, :n], axis=0, keepdims=True)

    front = dot(value, f_ref[...])
    wide = out_ref.shape[1] // 2
    part[0:4, :] = e_ref[0:4, :]
    put(4, front, dot(out_ref[:, wide:], h_ref[...]))
    put(6, front, dot(out_ref[:, :wide], g_ref[...]))

    near = [(me_s, ranks[d]) for d in range(1, R)]
    across = [((me_s + d) % S, me_r) for d in range(1, S)]
    first = [send(part, land1.at[d], s1.at[d], r1.at[d], near[d]) for d in range(R - 1)]
    for copy in first:
        copy.start()
    value = part[...]
    for d in range(R - 1):
        first[d].wait_recv()
        value = value + land1[d]
    half[...] = value
    second = [send(half, far.at[d], s2.at[d], r2.at[d], across[d]) for d in range(S - 1)]
    for copy in second:
        copy.start()
    for d in range(S - 1):
        second[d].wait_recv()
        value = value + far[d]
    sum_ref[...] = value
    for copy in first + second:
        copy.wait_send()


def meet(S, R, u, w, f, g, h, e):
    return call(
        functools.partial(meet_kernel, S, R),
        [e.shape],
        [
            pltpu.VMEM((R,) + u.shape[1:], jnp.float32),
            pltpu.VMEM(w.shape[1:], jnp.float32),
            pltpu.SemaphoreType.DMA((S * R,)),
            pltpu.SemaphoreType.DMA((R,)),
            pltpu.SemaphoreType.DMA((S,)),
            pltpu.SemaphoreType.DMA((1,)),
            pltpu.VMEM(e.shape, jnp.float32),
            pltpu.VMEM((R - 1,) + e.shape, jnp.float32),
            pltpu.VMEM(e.shape, jnp.float32),
            pltpu.VMEM((S - 1,) + e.shape, jnp.float32),
            pltpu.SemaphoreType.DMA((R - 1,)),
            pltpu.SemaphoreType.DMA((R - 1,)),
            pltpu.SemaphoreType.DMA((S - 1,)),
            pltpu.SemaphoreType.DMA((S - 1,)),
        ],
        2,
        u,
        w,
        f,
        g,
        h,
        e,
    )[0]


def local(bitstrings, boundary, stem_tensor, probe_vectors, inbound_permutations):
    section = lax.axis_index("section")
    sections = lax.axis_size("section")
    rank = lax.axis_index("stem")
    rows, settings, width = stem_tensor.shape[2:]
    bonds = boundary.shape[1]
    micro, batch, qubits = bitstrings.shape[1:]
    count = micro * batch
    powers = jnp.left_shift(jnp.int32(1), jnp.arange(qubits, dtype=jnp.int32))
    own_setting = jnp.sum(bitstrings[0] * powers, axis=-1).reshape(count)
    ranks = lax.axis_size("stem")
    probe = probe_vectors[0]
    perm = inbound_permutations

    def flat(plane):
        return stem_tensor[0, plane].reshape(rows * settings, width)

    def own_rows(row):
        return lax.dynamic_slice_in_dim(row, rank * rows, rows)

    zeros_a = jnp.zeros((2 * settings, bonds), jnp.float32)

    def first_forward():
        t_re, t_im = stem_tensor[0, 0], stem_tensor[0, 1]
        b = jnp.dot(
            boundary,
            (jnp.arange(bonds, dtype=jnp.int32)[:, None] == own_rows(perm[0])[None, :]).astype(jnp.float32),
            precision=HIGHEST,
        )
        b_re, b_im = b[0][:, None, None], b[1][:, None, None]
        u_re = jnp.sum(b_re * t_re - b_im * t_im, axis=0)
        u_im = jnp.sum(b_re * t_im + b_im * t_re, axis=0)
        return jnp.concatenate([u_re, u_im])

    def last_backward():
        t_re, t_im = stem_tensor[0, 0], stem_tensor[0, 1]
        v_re = jnp.sum(t_re * probe[0] - t_im * probe[1], axis=-1)
        v_im = jnp.sum(t_re * probe[1] + t_im * probe[0], axis=-1)
        v = jnp.concatenate([v_re.T, v_im.T])
        return lax.dynamic_update_slice_in_dim(zeros_a, v, rank * rows, 1)

    idle = lambda: zeros_a
    vectors = lax.switch(section, [first_forward, idle, idle, last_backward])

    own_vectors = vectors
    blocks = vectors.reshape(2 * settings, ranks, rows).transpose(1, 0, 2)
    own_block = jnp.broadcast_to(own_setting.astype(jnp.float32), (8, count))
    blocks, setting = exchange(sections, ranks, blocks, own_block)
    setting = setting[:, 0].astype(jnp.int32)
    vectors = blocks.transpose(1, 0, 2).reshape(2 * settings, bonds)

    ends = settings + 1
    pairs = settings * settings
    zeros_u = jnp.zeros((bonds, 2 * pairs), jnp.float32)
    zeros_w = jnp.zeros((rows, 4 * pairs), jnp.float32)
    zeros_p = jnp.zeros((2, count), jnp.float32)

    def onehot(ids, size):
        return (jnp.arange(size, dtype=jnp.int32)[:, None] == ids[None, :]).astype(jnp.float32)

    def twice(pick):
        return jnp.kron(jnp.eye(2, dtype=jnp.float32), pick)

    front = onehot(setting[0] * settings + setting[1], pairs)

    def with_probe(v, pick):
        m = lax.dot_general(v, probe, (((1,), (1,)), ((), ())), precision=HIGHEST)
        n = m.shape[0] // 2
        amp = jnp.stack([m[:n, 0] - m[n:, 1], m[:n, 1] + m[n:, 0]])
        return jnp.dot(amp, pick, precision=HIGHEST)

    def first_amplitudes():
        return zeros_u, zeros_w, with_probe(own_vectors, onehot(setting[0], settings))

    def second_forward():
        x = select_columns(vectors, jnp.repeat(own_rows(perm[1]), settings))
        same = jnp.arange(rows * settings, dtype=jnp.int32)[None, :] % settings
        same = (same == jnp.arange(settings, dtype=jnp.int32)[:, None]).astype(jnp.float32)
        spread = (x[:, None, :] * same[None]).reshape(2 * pairs, rows * settings)
        p_re = jnp.dot(spread, flat(0), precision=HIGH)
        p_im = jnp.dot(spread, flat(1), precision=HIGH)
        u_re = p_re[:pairs] - p_im[pairs:]
        u_im = p_im[:pairs] + p_re[pairs:]
        u = jnp.concatenate([u_re, u_im])
        amp = with_probe(u, front)
        hi, lo = halves(u)
        pick = (perm[2][:, None] == jnp.arange(bonds, dtype=jnp.int32)[None, :]).astype(jnp.bfloat16)
        both = lax.dot_general(
            pick, jnp.concatenate([hi, lo]), (((1,), (1,)), ((), ())), preferred_element_type=jnp.float32
        )
        return both[:, : 2 * pairs] + both[:, 2 * pairs :], zeros_w, amp

    def second_backward():
        place = (perm[3][:, None] == jnp.arange(bonds, dtype=jnp.int32)[None, :]).astype(jnp.bfloat16)
        hi, lo = halves(vectors)
        both = jnp.dot(jnp.concatenate([hi, lo]), place, preferred_element_type=jnp.float32)
        v = (both[: 2 * settings] + both[2 * settings :]).reshape(2, settings, bonds)
        v = jnp.concatenate([v, probe[:, None, :]], axis=1).reshape(2 * ends, bonds)
        q_re = lax.dot_general(flat(0), v, (((1,), (1,)), ((), ())), precision=HIGH)
        q_im = lax.dot_general(flat(1), v, (((1,), (1,)), ((), ())), precision=HIGH)
        w_re = q_re[:, :ends] - q_im[:, ends:]
        w_im = q_re[:, ends:] + q_im[:, :ends]
        w_re, w_im = w_re.reshape(rows, settings, ends), w_im.reshape(rows, settings, ends)
        w = jnp.concatenate(
            [
                w_re[:, :, :settings].reshape(rows, pairs),
                w_im[:, :, :settings].reshape(rows, pairs),
                w_re[:, :, settings],
                w_im[:, :, settings],
                jnp.zeros((rows, 2 * pairs - 2 * settings), jnp.float32),
            ],
            axis=1,
        )
        return zeros_u, w, zeros_p

    none = lambda: (zeros_u, zeros_w, zeros_p)
    u, w, amp = lax.switch(section, [first_amplitudes, second_forward, second_backward, none])
    share = rows // sections
    unused = jnp.zeros((2 * (pairs - settings), 2 * count), jnp.float32)
    nothing = jnp.zeros_like(amp)
    summed = meet(
        sections,
        ranks,
        u.reshape(sections * ranks, share, 2 * pairs),
        w.reshape(sections, share, 4 * pairs),
        twice(front),
        twice(onehot(setting[2] * settings + setting[3], pairs)),
        jnp.concatenate([twice(onehot(setting[2], settings)), unused]),
        jnp.concatenate(
            [jnp.where(section == 0, amp, 0.0), jnp.where(section == 1, amp, 0.0), nothing, nothing]
        ),
    ).reshape(sections, 2, count)
    own = lax.dynamic_index_in_dim(summed, section, 0, False)
    return own.reshape(1, 2, micro, batch)


def solution(mesh):
    return jax.shard_map(
        local,
        mesh=mesh,
        in_specs=(
            P("section", None, None, None),
            P(),
            P("section", None, "stem", None, None),
            P("section", None, None),
            P(),
        ),
        out_specs=P("section", None, None, None),
        check_vma=False,
    )
```
